32 devices in a mesh: dp: 2 (over z, core), tp: 16 (over x, y).
Axes of the slice: x: 4, y: 4, z: 1, core: 2. Of those that a mesh axis runs over, the one named last changes fastest.
The devices are a block of a 4x4x8 slice.
Arguments:
- x: bfloat16 [8, 512, 4608], P('dp'), parts along dimension 0
- gain_a: bfloat16 [4608], replicated
- wq: bfloat16 [4608, 4096], P(None, 'tp')
- wk: bfloat16 [4608, 2048], P(None, 'tp')
- wv: bfloat16 [4608, 2048], P(None, 'tp')
- wo: bfloat16 [4096, 4608], P('tp')
- gain_m: bfloat16 [4608], replicated
- w_gate: bfloat16 [4608, 36864], P(None, 'tp')
- w_up: bfloat16 [4608, 36864], P(None, 'tp')
- w_down: bfloat16 [36864, 4608], P('tp')
Outputs:
- output: bfloat16 [8, 512, 4608], P('dp'), parts along dimension 0
There are 2 independent parts. The reference program is written for one: setup_inputs(seed, part) draws one part's arguments, and reference() takes and returns one part's arrays. A program takes and returns all parts, laid end to end along the dimension named above; an argument that names none is the same for every part.
All inputs are finite; a program needn't handle non-finite values.
Results may differ from the reference program's by a relative error of at most 0.017.
Values are sent between devices in bfloat16 or wider.
A program may use at most 768 MiB of HBM per device.

```python
import jax
import jax.numpy as jnp
from jax import lax

SEQUENCES = 4
TOKENS = 512
D = 4608
HEADS = 32
KV_HEADS = 16
HEAD = 128
FF = 36864
THETA = 10000


def setup_inputs(seed: int = 0, part: int = 0) -> dict:
    kx, ka, km, kq, kk, kv, ko, kg, ku, kd = jax.random.split(jax.random.key(seed), 10)

    def weights(key, rows, columns):
        return jax.random.normal(key, (rows, columns), jnp.float32) * rows**-0.5

    drawn = {
        "x": jax.random.normal(jax.random.fold_in(kx, part), (SEQUENCES, TOKENS, D), jnp.float32),
        "gain_a": 1 + 0.1 * jax.random.normal(ka, (D,), jnp.float32),
        "wq": 2 * weights(kq, D, HEADS * HEAD),
        "wk": 2 * weights(kk, D, KV_HEADS * HEAD),
        "wv": 4 * weights(kv, D, KV_HEADS * HEAD),
        "wo": weights(ko, HEADS * HEAD, D),
        "gain_m": 1 + 0.1 * jax.random.normal(km, (D,), jnp.float32),
        "w_gate": weights(kg, D, FF),
        "w_up": weights(ku, D, FF),
        "w_down": 3 * weights(kd, FF, D),
    }
    return {k: v.astype(jnp.bfloat16) for k, v in drawn.items()}


def normed(x, gain):
    wide = x.astype(jnp.float32)
    scale = lax.rsqrt(jnp.mean(wide * wide, -1, keepdims=True) + 1e-6)
    return (wide * scale * gain.astype(jnp.float32)).astype(jnp.bfloat16)


def turned(t, place, theta):
    half = t.shape[-1] // 2
    angle = place.astype(jnp.float32)[:, None] * theta ** (-jnp.arange(half, dtype=jnp.float32) / half)
    cos, sin = jnp.cos(angle)[:, None], jnp.sin(angle)[:, None]
    a, b = t[..., :half].astype(jnp.float32), t[..., half:].astype(jnp.float32)
    return jnp.concatenate([a * cos - b * sin, b * cos + a * sin], -1).astype(jnp.bfloat16)


def matmul(a, w):
    return jnp.dot(a, w, preferred_element_type=jnp.float32).astype(jnp.bfloat16)


def einsum(form, a, b):
    return jnp.einsum(form, a.astype(jnp.float32), b.astype(jnp.float32))


def attention(q, k, v):
    scores = einsum("tgsd,ugd->gstu", q, k) * q.shape[-1] ** -0.5
    token = jnp.arange(q.shape[0])
    scores = jnp.where(token[:, None] >= token, scores, -jnp.inf)
    weights = jax.nn.softmax(scores, -1).astype(jnp.bfloat16)
    return einsum("gstu,ugd->tgsd", weights, v).astype(jnp.bfloat16)


def one(x, gain_a, wq, wk, wv, wo, gain_m, w_gate, w_up, w_down):
    rows = x.shape[0]
    a, place = normed(x, gain_a), jnp.arange(rows)
    k = turned(matmul(a, wk).reshape(rows, -1, HEAD), place, THETA)
    q = turned(matmul(a, wq).reshape(rows, -1, HEAD), place, THETA).reshape(rows, k.shape[1], -1, HEAD)
    v = matmul(a, wv).reshape(rows, -1, HEAD)
    seen = attention(q, k, v).reshape(rows, -1)
    h = (x.astype(jnp.float32) + jnp.dot(seen, wo, preferred_element_type=jnp.float32)).astype(jnp.bfloat16)
    b = normed(h, gain_m)
    gate = jnp.dot(b, w_gate, preferred_element_type=jnp.float32)
    up = jnp.dot(b, w_up, preferred_element_type=jnp.float32)
    hidden = (jax.nn.silu(gate) * up).astype(jnp.bfloat16)
    return (h.astype(jnp.float32) + jnp.dot(hidden, w_down, preferred_element_type=jnp.float32)).astype(jnp.bfloat16)


def reference(x, gain_a, wq, wk, wv, wo, gain_m, w_gate, w_up, w_down):
    return lax.map(lambda sequence: one(sequence, gain_a, wq, wk, wv, wo, gain_m, w_gate, w_up, w_down), x)
```

```python
import functools

import jax
import jax.numpy as jnp
import numpy as np
from jax import lax
from jax.experimental import pallas as pl
from jax.experimental.pallas import tpu as pltpu
from jax.sharding import PartitionSpec as P

HEAD = 128
THETA = 10000
MESH = pl.DeviceIdType.MESH
LIMIT = 67043328
WIDE = 256


def _mod(x, n):
    return lax.rem(x + 4 * n, n)


def _layer(side, x, gain_a, wq, wk, wv, wo_in, cos, sin, gain, w_gate, w_up, w_down, y, partial, held, b, hidden, gbuf, dbuf, big, small,
           own, seen, heads, wo, big_send, big_recv, small_send, small_recv, fan_send, fan_recv, row_send, row_recv, gsem, dsem, osem, isem,
           xsem, ysem):
    batch, rows, d = x.shape
    f = w_gate.shape[1]
    jobs = 2 * batch
    part, quarter = rows // 2, d // 4
    group, block = part // side, part // side // side
    me = lax.axis_index("tp")
    px, py = lax.div(me, side), lax.rem(me, side)
    ways = []
    for k in range(4):
        step = 1 if k % 2 == 0 else -1
        on_x, on_y = _mod(px + step, side) * side + py, px * side + _mod(py + step, side)
        ways.append((step, px, py, on_x, on_y) if k < 2 else (step, py, px, on_y, on_x))

    def group_rows(q, g):
        return pl.ds(pl.multiple_of(q * part + g * group, group), group)

    def block_rows(q, g, m):
        return pl.ds(pl.multiple_of(q * part + g * group + m * block, block), block)

    def columns(k):
        return slice(k * quarter, (k + 1) * quarter)

    def send_big(j, q, k, s):
        at = lax.rem(j, 2)
        return pltpu.make_async_remote_copy(big.at[at, q, k, s], big.at[at, q, k, s + 1], big_send.at[q, k, s], big_recv.at[at, q, k, s],
                                            device_id={"tp": ways[k][3]}, device_id_type=MESH)

    def send_small(j, q, k, s):
        at = lax.rem(j, 2)
        return pltpu.make_async_remote_copy(small.at[at, q, k, s], small.at[at, q, k, s + 1], small_send.at[q, k, s],
                                            small_recv.at[at, q, k, s], device_id={"tp": ways[k][4]}, device_id_type=MESH)

    def fan(j, q, k, s):
        step, a, c, _, to = ways[k]
        at = lax.rem(j, 2)
        where = held.at[at, block_rows(q, a, _mod(c - step * s, side)), columns(k)]
        return pltpu.make_async_remote_copy(where, where, fan_send.at[q, k, s], fan_recv.at[at, q, k, s], device_id={"tp": to},
                                            device_id_type=MESH)

    def fan_rows(j, q, k, s):
        step, a, _, to, _ = ways[k]
        at = lax.rem(j, 2)
        where = held.at[at, group_rows(q, _mod(a - step * s, side)), columns(k)]
        return pltpu.make_async_remote_copy(where, where, row_send.at[q, k, s], row_recv.at[at, q, k, s], device_id={"tp": to},
                                            device_id_type=MESH)

    last = side - 2

    def reduce_big(j, q, s):
        at = lax.rem(j, 2)
        for k in range(4):
            step, a = ways[k][:2]
            mine = partial.at[at, group_rows(q, _mod(a - step * (s + 1), side)), columns(k)]

            @pl.when(s == 0)
            def _():
                big[at, q, k, 0] = mine[...].astype(jnp.bfloat16)

            @pl.when(s > 0)
            def _():
                send_big(j, q, k, s - 1).wait()
                big[at, q, k, s] = (big[at, q, k, s].astype(jnp.float32) + mine[...]).astype(jnp.bfloat16)

            send_big(j, q, k, s).start()

    def reduce_small(j, q, s):
        at = lax.rem(j, 2)
        for k in range(4):
            step, a, c = ways[k][:3]
            mine = partial.at[at, block_rows(q, a, _mod(c - step * (s + 1), side)), columns(k)]

            @pl.when(s == 0)
            def _():
                send_big(j, q, k, last).wait()
                whole = partial.at[at, group_rows(q, a), columns(k)]
                whole[...] = whole[...] + big[at, q, k, side - 1].astype(jnp.float32)
                small[at, q, k, 0] = mine[...].astype(jnp.bfloat16)

            @pl.when(s > 0)
            def _():
                send_small(j, q, k, s - 1).wait()
                small[at, q, k, s] = (small[at, q, k, s].astype(jnp.float32) + mine[...]).astype(jnp.bfloat16)

            send_small(j, q, k, s).start()

    def finish(j, q):
        at, seq = lax.rem(j, 2), lax.rem(j, batch)
        for k in range(4):
            _, a, c = ways[k][:3]
            send_small(j, q, k, last).wait()
            here = block_rows(q, a, c)
            total = small[at, q, k, side - 1].astype(jnp.float32) + partial[at, here, columns(k)]
            new = (own[seq, q, k].astype(jnp.float32) + total).astype(jnp.bfloat16)
            own[seq, q, k] = new
            held[at, here, columns(k)] = new
            fan(j, q, k, 0).start()

    def spread_small(j, q, s):
        for k in range(4):
            fan(j, q, k, s - 1).wait()
            fan(j, q, k, s).start()

    def spread_big(j, q, s):
        for k in range(4):
            @pl.when(s == 0)
            def _():
                fan(j, q, k, last).wait()

            @pl.when(s > 0)
            def _():
                fan_rows(j, q, k, s - 1).wait()

            fan_rows(j, q, k, s).start()

    def arrived(j, q):
        for k in range(4):
            fan_rows(j, q, k, last).wait()

    strip = rows // 16

    def scaled(wide, weight):
        scale = lax.rsqrt(jnp.mean(wide * wide, -1, keepdims=True) + 1e-6)
        return (wide * scale * weight[...].astype(jnp.float32)).astype(jnp.bfloat16)

    def fetch_x(seq):
        return pltpu.make_async_copy(x.at[seq], b, xsem)

    def norm_x(half):
        @pl.loop(0, 8)
        def _(t):
            here = pl.ds(pl.multiple_of(half * (rows // 2) + t * strip, strip), strip)
            b[here, :] = scaled(b[here, :].astype(jnp.float32), gain_a)

    def qkv(seq):
        for n in range(2):
            heads[n] = jnp.dot(b[...], gbuf[n], preferred_element_type=jnp.float32).astype(jnp.bfloat16)

        @pl.when(seq + 1 < batch)
        def _():
            fetch_x(seq + 1).start()

    def turned(t, here):
        wide = t.astype(jnp.float32)
        half = HEAD // 2
        return (wide * cos[here, :] + jnp.concatenate([wide[:, half:], wide[:, :half]], -1) * sin[here, :]).astype(jnp.bfloat16)

    tall = min(rows, 128)

    def attention(seq):
        for at in range(0, rows, tall):
            here = slice(at, at + tall)
            heads[1, here, :HEAD] = turned(heads[1, here, :HEAD], here)
        for at in range(0, rows, tall):
            here, end = slice(at, at + tall), at + tall
            hidden_key = (lax.broadcasted_iota(jnp.int32, (tall, end), 1) > at + lax.broadcasted_iota(jnp.int32, (tall, end), 0))
            for n in range(heads.shape[2] // HEAD):
                cols = slice(n * HEAD, (n + 1) * HEAD)
                scores = lax.dot_general(turned(heads[0, here, cols], here), heads[1, :end, :HEAD], (((1,), (1,)), ((), ())),
                                         preferred_element_type=jnp.float32) * HEAD**-0.5
                scores = jnp.where(hidden_key, -jnp.inf, scores)
                weights = jnp.exp(scores - jnp.max(scores, -1, keepdims=True))
                weights = (weights * (1 / jnp.sum(weights, -1, keepdims=True))).astype(jnp.bfloat16)
                seen[seq, here, cols] = jnp.dot(weights, heads[1, :end, HEAD:2 * HEAD], preferred_element_type=jnp.float32).astype(jnp.bfloat16)

    def project(seq):
        at = lax.rem(seq, 2)

        @pl.loop(0, d // WIDE)
        def _(t):
            cols = pl.ds(pl.multiple_of(t * WIDE, WIDE), WIDE)
            partial[at, :, cols] = jnp.dot(seen[seq], wo[:, cols], preferred_element_type=jnp.float32)

    def norm(seq, half):
        @pl.loop(0, 8)
        def _(t):
            here = pl.ds(pl.multiple_of(half * (rows // 2) + t * strip, strip), strip)
            b[here, :] = scaled(held[lax.rem(seq, 2), here, :].astype(jnp.float32), gain)

    n_up, n_down = f // 128, d // WIDE
    per_up, per_down = -(-n_up // 9), -(-n_down // 9)

    def fetch_up(n):
        at, cols = lax.rem(n, 2), pl.ds(pl.multiple_of(lax.rem(n, n_up) * 128, 128), 128)
        return (pltpu.make_async_copy(w_gate.at[:, cols], gbuf.at[at, :, 0:128], gsem.at[at, 0]),
                pltpu.make_async_copy(w_up.at[:, cols], gbuf.at[at, :, 128:256], gsem.at[at, 1]))

    def fetch_down(n):
        at, cols = lax.rem(n, 2), pl.ds(pl.multiple_of(lax.rem(n, n_down) * WIDE, WIDE), WIDE)
        return (pltpu.make_async_copy(w_down.at[:, cols], dbuf.at[at], dsem.at[at]),)

    def up(seq, t):
        n = seq * n_up + t
        for copy in fetch_up(n):
            copy.wait()

        @pl.when(n + 1 < batch * n_up)
        def _():
            for copy in fetch_up(n + 1):
                copy.start()

        both = jnp.dot(b[...], gbuf[lax.rem(n, 2)], preferred_element_type=jnp.float32)
        hidden[lax.rem(seq, 2), :, pl.ds(pl.multiple_of(t * 128, 128), 128)] = (
            jax.nn.silu(both[:, :128]) * both[:, 128:]).astype(jnp.bfloat16)

    def down(seq, t):
        n = seq * n_down + t
        for copy in fetch_down(n):
            copy.wait()

        @pl.when(n + 1 < batch * n_down)
        def _():
            for copy in fetch_down(n + 1):
                copy.start()

        partial[lax.rem(seq, 2), :, pl.ds(pl.multiple_of(t * WIDE, WIDE), WIDE)] = jnp.dot(
            hidden[lax.rem(seq, 2)], dbuf[lax.rem(n, 2)], preferred_element_type=jnp.float32)

    def put_out(j):
        return pltpu.make_async_copy(held.at[lax.rem(j, 2)], y.at[lax.rem(j, batch)], ysem)

    def residuals():
        for seq in range(batch):
            for q in range(2):
                for k in range(4):
                    _, a, c = ways[k][:3]
                    yield pltpu.make_async_copy(x.at[seq, block_rows(q, a, c), columns(k)], own.at[seq, q, k], osem.at[seq, q, k])

    projections = [pltpu.make_async_copy(wq, gbuf.at[0], isem.at[0]), pltpu.make_async_copy(wk, gbuf.at[1, :, :HEAD], isem.at[1]),
                   pltpu.make_async_copy(wv, gbuf.at[1, :, HEAD:2 * HEAD], isem.at[2])]
    output = pltpu.make_async_copy(wo_in, wo, isem.at[3])
    for copy in (fetch_x(0), *projections, output, *residuals(), *fetch_down(0)):
        copy.start()
    barrier = pltpu.get_barrier_semaphore()
    for k in range(4):
        pl.semaphore_signal(barrier, inc=1, device_id={"tp": ways[k][3]}, device_id_type=MESH)
    fetch_x(0).wait()
    norm_x(0)
    norm_x(1)
    for copy in projections:
        copy.wait()
    qkv(0)
    attention(0)
    for copy in (output, *residuals()):
        copy.wait()
    project(0)
    pl.semaphore_wait(barrier, 4)

    steps = 2 * (side - 1)
    slots = 2 * steps

    def turn(t, _):
        r, i = lax.div(t, slots), lax.rem(t, slots)
        p, q = lax.div(i, 2), lax.rem(i, 2)
        reducing, spreading = r < jobs, (r >= 1) & (r <= jobs)

        @pl.when(reducing & (p < side - 1))
        def _():
            reduce_big(r, q, p)

        @pl.when(reducing & (p >= side - 1))
        def _():
            reduce_small(r, q, p - (side - 1))

        @pl.when(spreading & (p == 0))
        def _():
            finish(r - 1, q)

        @pl.when((r >= 2) & (p == 0))
        def _():
            arrived(r - 2, q)

        @pl.when(spreading & (p >= 1) & (p < side - 1))
        def _():
            spread_small(r - 1, q, p)

        @pl.when(spreading & (p >= side - 1))
        def _():
            spread_big(r - 1, q, p - (side - 1))

        ahead, unit = 2 * r + 1 + lax.div(i + 4, 5) - 1, lax.rem(i + 4, 5)
        attending = (i >= 1) & (i <= 10) & (ahead < batch)

        @pl.when(attending & (unit == 0))
        def _():
            fetch_x(ahead).wait()

        @pl.when(attending & (unit < 2))
        def _():
            norm_x(unit)

        @pl.when(attending & (unit == 2))
        def _():
            qkv(ahead)

        @pl.when(attending & (unit == 3))
        def _():
            attention(ahead)

        @pl.when((r + 1 < batch) & (((r == 0) & (i == 5)) | ((r > 0) & (i == 1))))
        def _():
            project(r + 1)

        @pl.when((r == 2) & (i == 0))
        def _():
            for copy in fetch_up(0):
                copy.start()

        @pl.when((r >= 2) & (r < batch + 2) & (i >= 1) & (i <= 2))
        def _():
            norm(r - 2, i - 1)

        @pl.when((r >= 3) & (r < batch + 3) & (i >= 1) & (i <= 9))
        def _():
            @pl.loop(0, per_down)
            def _(u):
                tile = (i - 1) * per_down + u

                @pl.when(tile < n_down)
                def _():
                    down(r - 3, tile)

        @pl.when((r >= 2) & (r < batch + 2) & (i >= 3))
        def _():
            @pl.loop(0, per_up)
            def _(u):
                tile = (i - 3) * per_up + u

                @pl.when(tile < n_up)
                def _():
                    up(r - 2, tile)

        @pl.when((r >= batch + 2) & (i == 1))
        def _():
            put_out(r - 2).start()

        @pl.when((r >= batch + 2) & (r < jobs + 1) & (i == 5))
        def _():
            put_out(r - 2).wait()

        return 0

    lax.fori_loop(0, (jobs + 1) * slots + 2, turn, 0)
    put_out(jobs - 1).wait()


def layer(side, x, gain_a, wq, wk, wv, wo, gain, w_gate, w_up, w_down):
    batch, rows, d = x.shape
    f, mine = w_gate.shape[1], wq.shape[1]
    part, quarter = rows // 2, d // 4
    group, block = part // side, part // side // side
    low, dma = jnp.bfloat16, pltpu.SemaphoreType.DMA
    anywhere, vmem = pl.BlockSpec(memory_space=pl.ANY), pl.BlockSpec(memory_space=pltpu.VMEM)
    angle = np.arange(rows)[:, None] * float(THETA) ** (-np.arange(HEAD // 2) / (HEAD // 2))
    cos, sin = np.cos(angle).astype(np.float32), np.sin(angle).astype(np.float32)
    flops = 2 * batch * rows * d * (3 * f + 3 * mine)
    return pl.pallas_call(
        functools.partial(_layer, side),
        out_shape=jax.ShapeDtypeStruct(x.shape, low),
        in_specs=[anywhere, vmem, anywhere, anywhere, anywhere, anywhere, vmem, vmem, vmem, anywhere, anywhere, anywhere],
        out_specs=anywhere,
        scratch_shapes=[
            pltpu.VMEM((2, rows, d), jnp.float32),
            pltpu.VMEM((2, rows, d), low),
            pltpu.VMEM((rows, d), low),
            pltpu.VMEM((2, rows, f), low),
            pltpu.VMEM((2, d, 256), low),
            pltpu.VMEM((2, f, WIDE), low),
            pltpu.VMEM((2, 2, 4, side, group, quarter), low),
            pltpu.VMEM((2, 2, 4, side, block, quarter), low),
            pltpu.VMEM((batch, 2, 4, block, quarter), low),
            pltpu.VMEM((batch, rows, mine), low),
            pltpu.VMEM((2, rows, mine), low),
            pltpu.VMEM(wo.shape, low),
            *[dma(s) for _ in range(4) for s in ((2, 4, side - 1), (2, 2, 4, side - 1))],
            dma((2, 2)), dma((2,)), dma((batch, 2, 4)), dma((4,)), dma, dma,
        ],
        compiler_params=pltpu.CompilerParams(collective_id=0, has_side_effects=True, vmem_limit_bytes=LIMIT),
        cost_estimate=pl.CostEstimate(flops=flops, transcendentals=batch * rows * f, bytes_accessed=6 * batch * d * f),
    )(x, gain_a.reshape(1, d), wq, wk, wv, wo, jnp.asarray(np.concatenate([cos, cos], 1)), jnp.asarray(np.concatenate([-sin, sin], 1)),
      gain.reshape(1, d), w_gate, w_up, w_down)


def solution(mesh):
    side = round(mesh.shape["tp"] ** 0.5)
    tokens, whole, columns, rows_of = P("dp", None, None), P(None), P(None, "tp"), P("tp", None)
    return jax.shard_map(
        functools.partial(layer, side),
        mesh=mesh,
        in_specs=(tokens, whole, columns, columns, columns, rows_of, whole, columns, columns, rows_of),
        out_specs=tokens,
        check_vma=False,
    )
```

```python
import functools

import jax
import jax.numpy as jnp
import numpy as np
from jax import lax
from jax.experimental import pallas as pl
from jax.experimental.pallas import tpu as pltpu
from jax.sharding import PartitionSpec as P

HEAD = 128
THETA = 10000
LOG2E = 1.4426950408889634
MESH = pl.DeviceIdType.MESH
LIMIT = 67043328
WIDE = 512


def _mod(x, n):
    return lax.rem(x + 4 * n, n)


def _layer(side, x, gain_a, wq, wk, wv, wo_in, cos, sin, gain, w_gate, w_up, w_down, y, partial, held, b, hidden, gbuf, dbuf, big, small,
           big_own, small_own, own, big_send, big_recv, small_send, small_recv, fan_send, fan_recv, row_send, row_recv, gsem, dsem, osem, isem,
           wsem, xsem, ysem):
    batch, rows, d = x.shape
    f = w_gate.shape[1]
    jobs = 2 * batch
    part, quarter = rows // 2, d // 4
    group, block = part // side, part // side // side
    me = lax.axis_index("tp")
    px, py = lax.div(me, side), lax.rem(me, side)
    ways = []
    for k in range(4):
        step = 1 if k % 2 == 0 else -1
        on_x, on_y = _mod(px + step, side) * side + py, px * side + _mod(py + step, side)
        ways.append((step, px, py, on_x, on_y) if k < 2 else (step, py, px, on_y, on_x))

    def group_rows(q, g):
        return pl.ds(pl.multiple_of(q * part + g * group, group), group)

    def block_rows(q, g, m):
        return pl.ds(pl.multiple_of(q * part + g * group + m * block, block), block)

    def columns(k):
        return slice(k * quarter, (k + 1) * quarter)

    def send_big(j, q, k, s, source=None):
        at = lax.rem(j, 2)
        source = big_own.at[q, k] if source is None else source
        return pltpu.make_async_remote_copy(source, big.at[at, q, k, s], big_send.at[q, k, s], big_recv.at[at, q, k, s],
                                            device_id={"tp": ways[k][3]}, device_id_type=MESH)

    def send_small(j, q, k, s, source=None):
        at = lax.rem(j, 2)
        source = small_own.at[q, k] if source is None else source
        return pltpu.make_async_remote_copy(source, small.at[at, q, k, s], small_send.at[q, k, s], small_recv.at[at, q, k, s],
                                            device_id={"tp": ways[k][4]}, device_id_type=MESH)

    def fan(j, q, k, s):
        step, a, c, _, to = ways[k]
        at = lax.rem(j, 2)
        where = held.at[at, block_rows(q, a, _mod(c - step * s, side)), columns(k)]
        return pltpu.make_async_remote_copy(where, where, fan_send.at[q, k, s], fan_recv.at[at, q, k, s], device_id={"tp": to},
                                            device_id_type=MESH)

    def fan_rows(j, q, k, s):
        step, a, _, to, _ = ways[k]
        at = lax.rem(j, 2)
        where = held.at[at, group_rows(q, _mod(a - step * s, side)), columns(k)]
        return pltpu.make_async_remote_copy(where, where, row_send.at[q, k, s], row_recv.at[at, q, k, s], device_id={"tp": to},
                                            device_id_type=MESH)

    last = side - 2

    def reduce_big(j, q, s):
        at = lax.rem(j, 2)
        for k in range(4):
            step, a = ways[k][:2]
            mine = partial.at[at, group_rows(q, _mod(a - step * (s + 1), side)), columns(k)]

            @pl.when(s == 0)
            def _():
                big_own[q, k] = mine[...].astype(jnp.bfloat16)
                send_big(j, q, k, 0).start()

            @pl.when(s > 0)
            def _():
                send_big(j, q, k, s - 1).wait()
                big[at, q, k, s - 1] = (big[at, q, k, s - 1].astype(jnp.float32) + mine[...]).astype(jnp.bfloat16)
                send_big(j, q, k, s, big.at[at, q, k, s - 1]).start()

    def reduce_small(j, q, s):
        at = lax.rem(j, 2)
        for k in range(4):
            step, a, c = ways[k][:3]
            mine = partial.at[at, block_rows(q, a, _mod(c - step * (s + 1), side)), columns(k)]

            @pl.when(s == 0)
            def _():
                send_big(j, q, k, last).wait()
                whole = partial.at[at, group_rows(q, a), columns(k)]
                whole[...] = whole[...] + big[at, q, k, last].astype(jnp.float32)
                small_own[q, k] = mine[...].astype(jnp.bfloat16)
                send_small(j, q, k, 0).start()

            @pl.when(s > 0)
            def _():
                send_small(j, q, k, s - 1).wait()
                small[at, q, k, s - 1] = (small[at, q, k, s - 1].astype(jnp.float32) + mine[...]).astype(jnp.bfloat16)
                send_small(j, q, k, s, small.at[at, q, k, s - 1]).start()

    def finish(j, q):
        at, seq = lax.rem(j, 2), lax.rem(j, batch)
        for k in range(4):
            _, a, c = ways[k][:3]
            send_small(j, q, k, last).wait()
            here = block_rows(q, a, c)
            total = small[at, q, k, last].astype(jnp.float32) + partial[at, here, columns(k)]
            new = (own[seq, q, k].astype(jnp.float32) + total).astype(jnp.bfloat16)
            own[seq, q, k] = new
            held[at, here, columns(k)] = new
            fan(j, q, k, 0).start()

    def spread_small(j, q, s):
        for k in range(4):
            fan(j, q, k, s - 1).wait()
            fan(j, q, k, s).start()

    def spread_big(j, q, s):
        for k in range(4):
            @pl.when(s == 0)
            def _():
                fan(j, q, k, last).wait()

            @pl.when(s > 0)
            def _():
                fan_rows(j, q, k, s - 1).wait()

            fan_rows(j, q, k, s).start()

    def arrived(j, q):
        for k in range(4):
            fan_rows(j, q, k, last).wait()

    strip = rows // 16

    def scaled(wide, weight):
        scale = lax.rsqrt(jnp.mean(wide * wide, -1, keepdims=True) + 1e-6)
        return (wide * scale * weight[...].astype(jnp.float32)).astype(jnp.bfloat16)

    def fetch_x(seq):
        return pltpu.make_async_copy(x.at[seq], b, xsem)

    def turned(t, here):
        wide = t.astype(jnp.float32)
        half = HEAD // 2
        return (wide * cos[here, :] + jnp.concatenate([wide[:, half:], wide[:, :half]], -1) * sin[here, :]).astype(jnp.bfloat16)

    heads = hidden.at[1]
    share = wq.shape[1]

    def attention(seq, half):
        tall = rows // 2
        here, end = slice(half * tall, half * tall + tall), half * tall + tall

        @pl.loop(0, 8)
        def _(t):
            some = pl.ds(pl.multiple_of(half * tall + t * strip, strip), strip)
            b[some, :] = scaled(b[some, :].astype(jnp.float32), gain_a)

        heads[here, :2 * share] = jnp.dot(b[here, :], gbuf[0], preferred_element_type=jnp.float32).astype(jnp.bfloat16)
        key, value = slice(share, share + HEAD), slice(share + HEAD, share + 2 * HEAD)
        heads[here, key] = turned(heads[here, key], here)
        n = share // HEAD
        queries = jnp.concatenate([turned(heads[here, m * HEAD:(m + 1) * HEAD], here) for m in range(n)], 0)
        scores = lax.dot_general(queries, heads[:end, key], (((1,), (1,)), ((), ())), preferred_element_type=jnp.float32)
        place = half * tall + lax.rem(lax.broadcasted_iota(jnp.int32, (n * tall, end), 0), tall)
        scores = jnp.where(lax.broadcasted_iota(jnp.int32, (n * tall, end), 1) > place, -jnp.inf, scores)
        weights = jnp.exp2((scores - jnp.max(scores, -1, keepdims=True)) * (HEAD**-0.5 * LOG2E))
        total = jnp.sum(weights, -1, keepdims=True)
        out = (jnp.dot(weights.astype(jnp.bfloat16), heads[:end, value], preferred_element_type=jnp.float32) * (1 / total)).astype(jnp.bfloat16)
        for m in range(n):
            hidden[0, here, pl.ds(pl.multiple_of(seq * share + m * HEAD, HEAD), HEAD)] = out[m * tall:(m + 1) * tall]

    def project(seq, here):
        seen = hidden.at[0, here, pl.ds(pl.multiple_of(seq * share, share), share)]

        @pl.loop(0, d // WIDE)
        def _(t):
            cols = pl.ds(pl.multiple_of(t * WIDE, WIDE), WIDE)
            some = pl.ds(pl.multiple_of(t * share, share), share)
            partial[lax.rem(seq, 2), here, cols] = jnp.dot(seen[...], dbuf[1, some, :], preferred_element_type=jnp.float32)

    def norm(seq, half):
        @pl.loop(0, 8)
        def _(t):
            here = pl.ds(pl.multiple_of(half * (rows // 2) + t * strip, strip), strip)
            b[here, :] = scaled(held[lax.rem(seq, 2), here, :].astype(jnp.float32), gain)

    tall = WIDE // 2
    n_up, n_down = f // tall, d // WIDE

    def fetch_up(n):
        at, cols = lax.rem(n, 2), pl.ds(pl.multiple_of(lax.rem(n, n_up) * tall, tall), tall)
        return (pltpu.make_async_copy(w_gate.at[:, cols], gbuf.at[at, :, :tall], gsem.at[at, 0]),
                pltpu.make_async_copy(w_up.at[:, cols], gbuf.at[at, :, tall:], gsem.at[at, 1]))

    def fetch_down(n):
        at, cols = lax.rem(n, 2), pl.ds(pl.multiple_of(lax.rem(n, n_down) * WIDE, WIDE), WIDE)
        return (pltpu.make_async_copy(w_down.at[:, cols], dbuf.at[at], dsem.at[at]),)

    def up(seq, t):
        n = seq * n_up + t
        for copy in fetch_up(n):
            copy.wait()

        @pl.when(n + 1 < batch * n_up)
        def _():
            for copy in fetch_up(n + 1):
                copy.start()

        both = jnp.dot(b[...], gbuf[lax.rem(n, 2)], preferred_element_type=jnp.float32)
        hidden[lax.rem(seq, 2), :, pl.ds(pl.multiple_of(t * tall, tall), tall)] = (
            jax.nn.silu(both[:, :tall]) * both[:, tall:]).astype(jnp.bfloat16)

    def down(seq, t):
        n = seq * n_down + t
        for copy in fetch_down(n):
            copy.wait()

        @pl.when(n + 1 < batch * n_down)
        def _():
            for copy in fetch_down(n + 1):
                copy.start()

        partial[lax.rem(seq, 2), :, pl.ds(pl.multiple_of(t * WIDE, WIDE), WIDE)] = jnp.dot(
            hidden[lax.rem(seq, 2)], dbuf[lax.rem(n, 2)], preferred_element_type=jnp.float32)

    def put_out(j):
        return pltpu.make_async_copy(held.at[lax.rem(j, 2)], y.at[lax.rem(j, batch)], ysem)

    def residuals():
        for seq in range(batch):
            for q in range(2):
                for k in range(4):
                    _, a, c = ways[k][:3]
                    yield pltpu.make_async_copy(x.at[seq, block_rows(q, a, c), columns(k)], own.at[seq, q, k], osem.at[seq, q, k])

    projections = [pltpu.make_async_copy(wq, gbuf.at[0, :, :share], isem.at[0]),
                   pltpu.make_async_copy(wk, gbuf.at[0, :, share:share + HEAD], isem.at[1]),
                   pltpu.make_async_copy(wv, gbuf.at[0, :, share + HEAD:share + 2 * HEAD], isem.at[2])]
    output = [pltpu.make_async_copy(wo_in.at[:, t * WIDE:(t + 1) * WIDE], dbuf.at[1, t * share:(t + 1) * share, :], wsem.at[t])
              for t in range(d // WIDE)]
    for copy in (fetch_x(0), *projections, *output, *residuals(), *fetch_down(0)):
        copy.start()
    barrier = pltpu.get_barrier_semaphore()
    for k in range(4):
        pl.semaphore_signal(barrier, inc=1, device_id={"tp": ways[k][3]}, device_id_type=MESH)
    fetch_x(0).wait()
    for copy in projections:
        copy.wait()
    attention(0, 0)
    for copy in (*output, *residuals()):
        copy.wait()
    project(0, slice(0, rows // 2))
    pl.semaphore_wait(barrier, 4)

    steps = 2 * (side - 1)
    slots = 2 * steps

    def turn(t, _):
        r, i = lax.div(t, slots), lax.rem(t, slots)
        p, q = lax.div(i, 2), lax.rem(i, 2)
        reducing, spreading = r < jobs, (r >= 1) & (r <= jobs)

        @pl.when(reducing & (p < side - 1))
        def _():
            reduce_big(r, q, p)

        @pl.when(reducing & (p >= side - 1))
        def _():
            reduce_small(r, q, p - (side - 1))

        @pl.when(spreading & (p == 0))
        def _():
            finish(r - 1, q)

        @pl.when((r >= 2) & (p == 0))
        def _():
            arrived(r - 2, q)

        @pl.when(spreading & (p >= 1) & (p < side - 1))
        def _():
            spread_small(r - 1, q, p)

        @pl.when(spreading & (p >= side - 1))
        def _():
            spread_big(r - 1, q, p - (side - 1))

        ahead, unit = lax.div(i + 2, 3), lax.rem(i + 2, 3)
        attending = (r == 0) & (ahead < batch)

        @pl.when(attending & (i > 0) & (unit == 0))
        def _():
            fetch_x(ahead).wait()
            attention(ahead, 0)

        @pl.when(attending & ((unit == 1) | (i == 0)))
        def _():
            attention(ahead, 1)

            @pl.when(ahead + 1 < batch)
            def _():
                fetch_x(ahead + 1).start()

        @pl.when((r == 0) & (i == 0))
        def _():
            project(0, slice(rows // 2, rows))

        @pl.when((r + 1 < batch) & (((r == 0) & (i == 3)) | ((r > 0) & (i == 1))))
        def _():
            project(r + 1, slice(0, rows))

        @pl.when((r == 1) & (i == 1))
        def _():
            for copy in fetch_up(0):
                copy.start()

        @pl.when((r >= 2) & (r < batch + 2) & (i >= 1) & (i <= 2))
        def _():
            norm(r - 2, i - 1)

        @pl.when((r >= 3) & (r < batch + 3) & ((i == 2) | (lax.rem(i, 2) == 1)))
        def _():
            @pl.loop(0, 2)
            def _(u):
                tile = jnp.where(i < 3, 2 * (i - 1) + u, 4 + lax.div(i - 3, 2))

                @pl.when(((i < 3) | (u == 0)) & (tile < n_down))
                def _():
                    down(r - 3, tile)

        @pl.when((r >= 2) & (r < batch + 2) & (i >= 3) & (i - 3 < n_up))
        def _():
            up(r - 2, i - 3)

        @pl.when((r >= batch + 2) & (i == 1))
        def _():
            put_out(r - 2).start()

        @pl.when((r >= batch + 2) & (r < jobs + 1) & (i == 5))
        def _():
            put_out(r - 2).wait()

        return 0

    lax.fori_loop(0, (jobs + 1) * slots + 2, turn, 0)
    put_out(jobs - 1).wait()


def layer(side, x, gain_a, wq, wk, wv, wo, gain, w_gate, w_up, w_down):
    batch, rows, d = x.shape
    f, mine = w_gate.shape[1], wq.shape[1]
    part, quarter = rows // 2, d // 4
    group, block = part // side, part // side // side
    low, dma = jnp.bfloat16, pltpu.SemaphoreType.DMA
    anywhere, vmem = pl.BlockSpec(memory_space=pl.ANY), pl.BlockSpec(memory_space=pltpu.VMEM)
    angle = np.arange(rows)[:, None] * float(THETA) ** (-np.arange(HEAD // 2) / (HEAD // 2))
    cos, sin = np.cos(angle).astype(np.float32), np.sin(angle).astype(np.float32)
    flops = 2 * batch * rows * d * (3 * f + 3 * mine)
    return pl.pallas_call(
        functools.partial(_layer, side),
        out_shape=jax.ShapeDtypeStruct(x.shape, low),
        in_specs=[anywhere, vmem, anywhere, anywhere, anywhere, anywhere, vmem, vmem, vmem, anywhere, anywhere, anywhere],
        out_specs=anywhere,
        scratch_shapes=[
            pltpu.VMEM((2, rows, d), jnp.float32),
            pltpu.VMEM((2, rows, d), low),
            pltpu.VMEM((rows, d), low),
            pltpu.VMEM((2, rows, f), low),
            pltpu.VMEM((2, d, WIDE), low),
            pltpu.VMEM((2, f, WIDE), low),
            pltpu.VMEM((2, 2, 4, side - 1, group, quarter), low),
            pltpu.VMEM((2, 2, 4, side - 1, block, quarter), low),
            pltpu.VMEM((2, 4, group, quarter), low),
            pltpu.VMEM((2, 4, block, quarter), low),
            pltpu.VMEM((batch, 2, 4, block, quarter), low),
            *[dma(s) for _ in range(4) for s in ((2, 4, side - 1), (2, 2, 4, side - 1))],
            dma((2, 2)), dma((2,)), dma((batch, 2, 4)), dma((3,)), dma((d // WIDE,)), dma, dma,
        ],
        compiler_params=pltpu.CompilerParams(collective_id=0, has_side_effects=True, vmem_limit_bytes=LIMIT),
        cost_estimate=pl.CostEstimate(flops=flops, transcendentals=batch * rows * f, bytes_accessed=6 * batch * d * f),
    )(x, gain_a.reshape(1, d), wq, wk, wv, wo, jnp.asarray(np.concatenate([cos, cos], 1)), jnp.asarray(np.concatenate([-sin, sin], 1)),
      gain.reshape(1, d), w_gate, w_up, w_down)


def solution(mesh):
    side = round(mesh.shape["tp"] ** 0.5)
    tokens, whole, columns, rows_of = P("dp", None, None), P(None), P(None, "tp"), P("tp", None)
    return jax.shard_map(
        functools.partial(layer, side),
        mesh=mesh,
        in_specs=(tokens, whole, columns, columns, columns, rows_of, whole, columns, columns, rows_of),
        out_specs=tokens,
        check_vma=False,
    )
```

```python
import functools

import jax
import jax.numpy as jnp
import numpy as np
from jax import lax
from jax.experimental import pallas as pl
from jax.experimental.pallas import tpu as pltpu
from jax.sharding import PartitionSpec as P

HEAD = 128
THETA = 10000
LOG2E = 1.4426950408889634
MESH = pl.DeviceIdType.MESH
LIMIT = 67043328
WIDE = 512


def _mod(x, n):
    return lax.rem(x + 4 * n, n)


def _layer(side, x, x_blocks, gains, wq, wk, wv, wo_in, cos, sin, w_gate, w_up, w_down, y, partial, held, b, hidden, gbuf, dbuf, big, small,
           big_own, small_own, own, big_send, big_recv, small_send, small_recv, fan_send, fan_recv, row_send, row_recv, gsem, dsem, osem, isem,
           wo_send, wo_recv, see_send, see_recv, wsem, xsem, ysem):
    batch, rows, d = x.shape
    f = w_gate.shape[1]
    jobs = 2 * batch
    part, quarter = rows // 2, d // 4
    group, block = part // side, part // side // side
    me = lax.axis_index("tp")
    px, py = lax.div(me, side), lax.rem(me, side)
    ways = []
    for k in range(4):
        step = 1 if k % 2 == 0 else -1
        on_x, on_y = _mod(px + step, side) * side + py, px * side + _mod(py + step, side)
        ways.append((step, px, py, on_x, on_y) if k < 2 else (step, py, px, on_y, on_x))

    def group_rows(q, g):
        return pl.ds(pl.multiple_of(q * part + g * group, group), group)

    def block_rows(q, g, m):
        return pl.ds(pl.multiple_of(q * part + g * group + m * block, block), block)

    def columns(k):
        return slice(k * quarter, (k + 1) * quarter)

    def send_big(j, q, k, s, source=None):
        at = lax.rem(j, 2)
        source = big_own.at[q, k] if source is None else source
        return pltpu.make_async_remote_copy(source, big.at[at, q, k, s], big_send.at[q, k, s], big_recv.at[at, q, k, s],
                                            device_id={"tp": ways[k][3]}, device_id_type=MESH)

    def send_small(j, q, k, s, source=None):
        at = lax.rem(j, 2)
        source = small_own.at[q, k] if source is None else source
        return pltpu.make_async_remote_copy(source, small.at[at, q, k, s], small_send.at[q, k, s], small_recv.at[at, q, k, s],
                                            device_id={"tp": ways[k][4]}, device_id_type=MESH)

    def fan(j, q, k, s):
        step, a, c, _, to = ways[k]
        at = lax.rem(j, 2)
        where = held.at[at, block_rows(q, a, _mod(c - step if s == 1 else c, side)), columns(k)]
        to = ways[k ^ 1][4] if s == 2 else to
        return pltpu.make_async_remote_copy(where, where, fan_send.at[q, k, s], fan_recv.at[at, q, k, s], device_id={"tp": to},
                                            device_id_type=MESH)

    def fan_rows(j, q, k, s):
        step, a, _, to, _ = ways[k]
        at = lax.rem(j, 2)
        where = held.at[at, group_rows(q, _mod(a - step * s, side)), columns(k)]
        return pltpu.make_async_remote_copy(where, where, row_send.at[q, k, s], row_recv.at[at, q, k, s], device_id={"tp": to},
                                            device_id_type=MESH)

    last = side - 2

    def reduce_big(j, q, s):
        at = lax.rem(j, 2)
        for k in range(4):
            step, a = ways[k][:2]
            mine = partial.at[at, group_rows(q, _mod(a - step * (s + 1), side)), columns(k)]

            @pl.when(s == 0)
            def _():
                big_own[q, k] = mine[...].astype(jnp.bfloat16)
                send_big(j, q, k, 0).start()

            @pl.when(s > 0)
            def _():
                send_big(j, q, k, s - 1).wait()
                big[at, q, k, s - 1] = (big[at, q, k, s - 1].astype(jnp.float32) + mine[...]).astype(jnp.bfloat16)
                send_big(j, q, k, s, big.at[at, q, k, s - 1]).start()

    def reduce_small(j, q, s):
        at = lax.rem(j, 2)
        for k in range(4):
            step, a, c = ways[k][:3]
            mine = partial.at[at, block_rows(q, a, _mod(c - step * (s + 1), side)), columns(k)]

            @pl.when(s == 0)
            def _():
                send_big(j, q, k, last).wait()
                whole = partial.at[at, group_rows(q, a), columns(k)]
                whole[...] = whole[...] + big[at, q, k, last].astype(jnp.float32)
                small_own[q, k] = mine[...].astype(jnp.bfloat16)
                send_small(j, q, k, 0).start()

            @pl.when(s > 0)
            def _():
                send_small(j, q, k, s - 1).wait()
                small[at, q, k, s - 1] = (small[at, q, k, s - 1].astype(jnp.float32) + mine[...]).astype(jnp.bfloat16)
                send_small(j, q, k, s, small.at[at, q, k, s - 1]).start()

    def finish(j, q):
        at, seq = lax.rem(j, 2), lax.rem(j, batch)
        for k in range(4):
            _, a, c = ways[k][:3]
            send_small(j, q, k, last).wait()
            here = block_rows(q, a, c)
            total = small[at, q, k, last].astype(jnp.float32) + partial[at, here, columns(k)]
            new = (own[seq, q, k].astype(jnp.float32) + total).astype(jnp.bfloat16)
            own[seq, q, k] = new
            held[at, here, columns(k)] = new
        for k in range(4):
            fan(j, q, k, 0).start()
            fan(j, q, k, 2).start()

    def spread_small(j, q):
        for k in range(4):
            fan(j, q, k, 0).wait()
            fan(j, q, k, 1).start()

    def spread_big(j, q, s):
        for k in range(4):
            @pl.when(s == 0)
            def _():
                fan(j, q, k, 1).wait()
                fan(j, q, k, 2).wait()

            @pl.when(s > 0)
            def _():
                fan_rows(j, q, k, s - 1).wait()

            fan_rows(j, q, k, s).start()

    def arrived(j, q):
        for k in range(4):
            fan_rows(j, q, k, last).wait()

    off = w_gate.shape[1] - batch * wq.shape[1]

    def pair(e):
        return slice(2 * e, 2 * e + 2)

    def pair_rows(q, g, e):
        return pl.ds(pl.multiple_of(q * part + g * group + e * 2 * block, 2 * block), 2 * block)

    def quarter_at(g):
        return pl.ds(pl.multiple_of(g * quarter, quarter), quarter)

    def remote(source, target, send, recv, to):
        return pltpu.make_async_remote_copy(source, target, send, recv, device_id={"tp": to}, device_id_type=MESH)

    def wo_at(q, n):
        return big.at[n // 3, q, :, n % 3]

    def wo_copy(q, e, s):
        step, a, _, to, _ = ways[2 * q + e]
        sems = wo_send.at[q, e, s], wo_recv.at[q, e, s]
        relay = big.at[1, q, pair(e), 1]
        if s == 0:
            return remote(wo_in.at[pair(e), :, quarter_at(_mod(a + 2, side))], relay, *sems, to)
        if s == 1:
            return remote(wo_in.at[:, :, quarter_at(_mod(a + step, side))], wo_at(q, 1 + e), *sems, to)
        return remote(relay, big.at[1, q, pair(e), 0], *sems, to)

    def see(j, q, e, s):
        at, to, share = lax.rem(j, 2), ways[2 * q + e][3], wq.shape[1]
        sems = see_send.at[q, e, s], see_recv.at[at, q, e, s]
        near, far = slice(q * part, q * part + part), slice((2 + q) * part, (3 + q) * part)
        if s == 0:
            mine = hidden.at[0, near, pl.ds(pl.multiple_of(off + j * share, share), share)]
            return remote(mine, dbuf.at[at, near, e * share:(e + 1) * share], *sems, to)
        half = share // 2
        return remote(dbuf.at[at, near, e * (share + half):e * (share + half) + half], dbuf.at[at, far, e * half:(e + 1) * half], *sems, to)

    def see_more(j, q):
        for e in range(2):
            see(j, q, e, 0).wait()
            see(j, q, e, 1).start()

    def project(j, q):
        at, share = lax.rem(j, 2), wq.shape[1]
        for e in range(2):
            see(j, q, e, 1).wait()
        near, far = slice(q * part, q * part + part), slice((2 + q) * part, (3 + q) * part)
        seen = [hidden.at[0, near, pl.ds(pl.multiple_of(off + j * share, share), share)], dbuf.at[at, near, :share],
                dbuf.at[at, near, share:2 * share], dbuf.at[at, far, :share]]
        width = quarter // 3

        for t in range(3):
            cols = slice(t * width, (t + 1) * width)
            total = 0
            for n in range(4):
                total += jnp.dot(seen[n][...], big[n // 3, q, :, n % 3, :, cols].reshape(share, width), preferred_element_type=jnp.float32)
            partial[at, near, cols] = total

    def send_pair(j, q, e, s):
        at = lax.rem(j, 2)
        source = small_own.at[q, pair(e)] if s == 0 else small.at[at, q, pair(e), s - 1]
        return remote(source, small.at[at, q, pair(e), s], small_send.at[q, 2 * e, s], small_recv.at[at, q, 2 * e, s], ways[2 * q + e][4])

    def reduce_pairs(j, q, s):
        at = lax.rem(j, 2)
        for e in range(2):
            step, _, c = ways[2 * q + e][:3]
            mine = partial[at, pair_rows(q, _mod(c - step * (s + 1), side), e), :quarter].reshape(2, block, quarter)
            if s == 0:
                small_own[q, pair(e)] = mine.astype(jnp.bfloat16)
            else:
                send_pair(j, q, e, s - 1).wait()
                small[at, q, pair(e), s - 1] = (small[at, q, pair(e), s - 1].astype(jnp.float32) + mine).astype(jnp.bfloat16)
            send_pair(j, q, e, s).start()

    def fan_pair(j, q, e, s):
        step, a, c, _, to = ways[2 * q + e]
        at = lax.rem(j, 2)
        where = held.at[at, pair_rows(q, _mod(c - step if s == 1 else c, side), e), quarter_at(a)]
        to = ways[2 * q + 1 - e][4] if s == 2 else to
        return remote(where, where, fan_send.at[q, e, s], fan_recv.at[at, q, e, s], to)

    def fan_quarter(j, q, e, s, u):
        step, a, _, to, _ = ways[2 * q + e]
        at = lax.rem(j, 2)
        where = held.at[at, pl.ds(q * part + (2 * e + u) * (part // 4), part // 4), quarter_at(_mod(a - step * s, side))]
        return remote(where, where, row_send.at[q, 2 * e + u, s], row_recv.at[at, q, 2 * e + u, s], to)

    def finish_pairs(j, q):
        at = lax.rem(j, 2)
        for e in range(2):
            _, a, c = ways[2 * q + e][:3]
            send_pair(j, q, e, last).wait()
            here = pair_rows(q, c, e)
            total = small[at, q, pair(e), last].astype(jnp.float32).reshape(2 * block, quarter) + partial[at, here, :quarter]
            old = own[j, q, pair(e)].astype(jnp.float32).reshape(2 * block, quarter)
            held[at, here, quarter_at(a)] = (old + total).astype(jnp.bfloat16)
        for e in range(2):
            fan_pair(j, q, e, 0).start()
            fan_pair(j, q, e, 2).start()

    def spread_pairs(j, q):
        for e in range(2):
            fan_pair(j, q, e, 0).wait()
            fan_pair(j, q, e, 1).start()

    def have_quarter(j, q):
        for e in range(2):
            fan_pair(j, q, e, 1).wait()
            fan_pair(j, q, e, 2).wait()

    def spread_quarters(j, q, s, u):
        for e in range(2):
            if s > 0:
                fan_quarter(j, q, e, s - 1, u).wait()
            fan_quarter(j, q, e, s, u).start()

    def arrived_quarters(j, q):
        for e in range(2):
            for u in range(2):
                fan_quarter(j, q, e, last, u).wait()
        for k in range(4):
            _, a, c = ways[k][:3]
            own[j, q, k] = held[lax.rem(j, 2), block_rows(q, a, c), columns(k)]

    strip = rows // 16

    def scaled(wide, weight):
        scale = lax.rsqrt(jnp.mean(wide * wide, -1, keepdims=True) + 1e-6)
        return (wide * scale * gains[weight:weight + 1, :].astype(jnp.float32)).astype(jnp.bfloat16)

    def fetch_x(seq):
        return pltpu.make_async_copy(x.at[seq], held.at[lax.rem(seq, 2)], xsem.at[lax.rem(seq, 2)])

    def turned(t, here):
        wide = t.astype(jnp.float32)
        half = HEAD // 2
        return (wide * cos[here, :] + jnp.concatenate([wide[:, half:], wide[:, :half]], -1) * sin[here, :]).astype(jnp.bfloat16)

    heads = hidden.at[1]
    share = wq.shape[1]

    def attention(seq, half):
        tall = rows // 2
        here, end = slice(half * tall, half * tall + tall), half * tall + tall

        @pl.loop(0, 8)
        def _(t):
            some = pl.ds(pl.multiple_of(half * tall + t * strip, strip), strip)
            b[some, :] = scaled(held[lax.rem(seq, 2), some, :].astype(jnp.float32), 0)

        heads[here, :2 * share] = jnp.dot(b[here, :], gbuf[0], preferred_element_type=jnp.float32).astype(jnp.bfloat16)
        key, value = slice(share, share + HEAD), slice(share + HEAD, share + 2 * HEAD)
        heads[here, key] = turned(heads[here, key], here)
        n = share // HEAD
        queries = jnp.concatenate([turned(heads[here, m * HEAD:(m + 1) * HEAD], here) for m in range(n)], 0)
        scores = lax.dot_general(queries, heads[:end, key], (((1,), (1,)), ((), ())), preferred_element_type=jnp.float32)
        place = half * tall + lax.rem(lax.broadcasted_iota(jnp.int32, (n * tall, end), 0), tall)
        scores = jnp.where(lax.broadcasted_iota(jnp.int32, (n * tall, end), 1) > place, -jnp.inf, scores)
        weights = jnp.exp2((scores - jnp.max(scores, -1, keepdims=True)) * (HEAD**-0.5 * LOG2E))
        total = jnp.sum(weights, -1, keepdims=True)
        out = (jnp.dot(weights.astype(jnp.bfloat16), heads[:end, value], preferred_element_type=jnp.float32) * (1 / total)).astype(jnp.bfloat16)
        for m in range(n):
            hidden[0, here, pl.ds(pl.multiple_of(off + seq * share + m * HEAD, HEAD), HEAD)] = out[m * tall:(m + 1) * tall]

    def norm(seq, half):
        @pl.loop(0, 8)
        def _(t):
            here = pl.ds(pl.multiple_of(half * (rows // 2) + t * strip, strip), strip)
            b[here, :] = scaled(held[lax.rem(seq, 2), here, :].astype(jnp.float32), 1)

    tall = WIDE // 2
    n_up, n_down = f // tall, d // WIDE

    def fetch_up(n):
        at, cols = lax.rem(n, 2), pl.ds(pl.multiple_of(lax.rem(n, n_up) * tall, tall), tall)
        return (pltpu.make_async_copy(w_gate.at[:, cols], gbuf.at[at, :, :tall], gsem.at[at, 0]),
                pltpu.make_async_copy(w_up.at[:, cols], gbuf.at[at, :, tall:], gsem.at[at, 1]))

    def fetch_down(n):
        at, cols = lax.rem(n, 2), pl.ds(pl.multiple_of(lax.rem(n, n_down) * WIDE, WIDE), WIDE)
        return (pltpu.make_async_copy(w_down.at[:, cols], dbuf.at[at], dsem.at[at]),)

    def up(seq, t):
        n = seq * n_up + t
        for copy in fetch_up(n):
            copy.wait()

        @pl.when(n + 1 < batch * n_up)
        def _():
            for copy in fetch_up(n + 1):
                copy.start()

        both = jnp.dot(b[...], gbuf[lax.rem(n, 2)], preferred_element_type=jnp.float32)
        hidden[lax.rem(seq, 2), :, pl.ds(pl.multiple_of(t * tall, tall), tall)] = (
            jax.nn.silu(both[:, :tall]) * both[:, tall:]).astype(jnp.bfloat16)

    def down(seq, t):
        n = seq * n_down + t
        for copy in fetch_down(n):
            copy.wait()

        @pl.when(n + 1 < batch * n_down)
        def _():
            for copy in fetch_down(n + 1):
                copy.start()

        partial[lax.rem(seq, 2), :, pl.ds(pl.multiple_of(t * WIDE, WIDE), WIDE)] = jnp.dot(
            hidden[lax.rem(seq, 2)], dbuf[lax.rem(n, 2)], preferred_element_type=jnp.float32)

    def put_out(j):
        return pltpu.make_async_copy(held.at[lax.rem(j, 2)], y.at[lax.rem(j, batch)], ysem)

    def residuals():
        for seq in range(batch):
            for q in range(2):
                for e in range(2):
                    _, a, c = ways[2 * q + e][:3]
                    first = q * (part // block) + c * (group // block) + 2 * e
                    yield pltpu.make_async_copy(x_blocks.at[seq, pl.ds(first, 2), :, quarter_at(a)], own.at[seq, q, pair(e)], osem.at[seq, q, e])

    projections = [pltpu.make_async_copy(wq, gbuf.at[0, :, :share], isem.at[0]),
                   pltpu.make_async_copy(wk, gbuf.at[0, :, share:share + HEAD], isem.at[1]),
                   pltpu.make_async_copy(wv, gbuf.at[0, :, share + HEAD:share + 2 * HEAD], isem.at[2])]
    output = [pltpu.make_async_copy(wo_in.at[:, :, quarter_at(ways[2 * q][1])], wo_at(q, 0), wsem.at[q]) for q in range(2)]
    barrier = pltpu.get_barrier_semaphore()
    for k in range(4):
        pl.semaphore_signal(barrier, inc=1, device_id={"tp": ways[k][3]}, device_id_type=MESH)
    for copy in (fetch_x(0), *projections, fetch_x(1), *output, *residuals()):
        copy.start()
    both = [(q, e) for q in range(2) for e in range(2)]
    pl.semaphore_wait(barrier, 4)
    for s in range(2):
        for q, e in both:
            wo_copy(q, e, s).start()
    fetch_x(0).wait()
    for copy in projections:
        copy.wait()
    for q in range(2):
        attention(0, q)
        for e in range(2):
            see(0, q, e, 0).start()
    for q, e in both:
        wo_copy(q, e, 0).wait()
        wo_copy(q, e, 2).start()

    @pl.loop(1, batch)
    def _(seq):
        @pl.when(seq + 1 < batch)
        def _():
            fetch_x(seq + 1).start()

        fetch_x(seq).wait()
        for q in range(2):
            attention(seq, q)

        @pl.when(seq == batch - 2)
        def _():
            for q in range(2):
                see_more(0, q)

    for copy in fetch_up(0):
        copy.start()
    for copy in (*output, *residuals()):
        copy.wait()
    for q, e in both:
        wo_copy(q, e, 1).wait()
        wo_copy(q, e, 2).wait()
    for q in range(2):
        project(0, q)

    steps = 2 * (side - 1)
    slots = 2 * steps

    def turn(t, _):
        r, i = lax.div(t, slots), lax.rem(t, slots)
        p, q = lax.div(i, 2), lax.rem(i, 2)
        reducing, spreading = r < jobs, (r >= 1) & (r <= jobs)

        @pl.when(reducing & (r >= batch) & (p < side - 1))
        def _():
            reduce_big(r, q, p)

        @pl.when(reducing & (r >= batch) & (p >= side - 1))
        def _():
            reduce_small(r, q, p - (side - 1))

        @pl.when(spreading & (r > batch) & (p == 0))
        def _():
            finish(r - 1, q)

        @pl.when((r >= batch + 2) & (p == 0))
        def _():
            arrived(r - 2, q)

        @pl.when(spreading & (r > batch) & (p == 1))
        def _():
            spread_small(r - 1, q)

        @pl.when(spreading & (r > batch) & (p >= side - 1))
        def _():
            spread_big(r - 1, q, p - (side - 1))

        def each(condition, do):
            for half in range(2):
                @pl.when(condition & (q == half))
                def _():
                    do(half)

        for s in range(side - 1):
            each((r < batch) & (p == side - 1 + s), lambda half: reduce_pairs(r, half, s))
        each((r >= 1) & (r <= batch) & (p == 0), lambda half: finish_pairs(r - 1, half))
        each((r >= 2) & (r < batch + 2) & (p == 1), lambda half: arrived_quarters(r - 2, half))
        each((r >= 1) & (r <= batch) & (p == 1), lambda half: spread_pairs(r - 1, half))
        each((r >= 1) & (r <= batch) & (p == 2), lambda half: have_quarter(r - 1, half))

        def spread_both(half, s):
            spread_quarters(r - 1, half, s, 0)
            spread_quarters(r - 1, 1 - half, s, 1)

        for s in range(side - 1):
            each((r >= 1) & (r <= batch) & (p == side - 1 + s), lambda half: spread_both(half, s))

        def start_seeing(half):
            for e in range(2):
                see(r + 1, half, e, 0).start()

        each((r + 1 < batch) & (p == 0), start_seeing)
        each((r + 1 < batch) & (p == 1), lambda half: see_more(r + 1, half))
        each((r + 1 < batch) & (p == 2), lambda half: project(r + 1, half))

        @pl.when((r == 2) & (i == slots - 1))
        def _():
            for copy in fetch_down(0):
                copy.start()

        @pl.when((r >= 2) & (r < batch + 2) & (p == 1))
        def _():
            norm(r - 2, q)

        @pl.when((r >= 3) & (r < batch + 3) & ((i == 2) | (lax.rem(i, 2) == 1)))
        def _():
            @pl.loop(0, 2)
            def _(u):
                tile = jnp.where(i < 3, 2 * (i - 1) + u, 4 + lax.div(i - 3, 2))

                @pl.when(((i < 3) | (u == 0)) & (tile < n_down))
                def _():
                    down(r - 3, tile)

        @pl.when((r >= 2) & (r < batch + 2) & (i >= 4))
        def _():
            @pl.loop(0, 2)
            def _(u):
                tile = i - 4 + u

                @pl.when(((u == 0) | (i == slots - 1)) & (tile < n_up))
                def _():
                    up(r - 2, tile)

        @pl.when((r >= batch + 2) & (i == 1))
        def _():
            put_out(r - 2).start()

        @pl.when((r >= batch + 2) & (r < jobs + 1) & (i == 5))
        def _():
            put_out(r - 2).wait()

        return 0

    lax.fori_loop(0, (jobs + 1) * slots + 2, turn, 0)
    put_out(jobs - 1).wait()


def layer(side, x, gain_a, wq, wk, wv, wo, gain, w_gate, w_up, w_down):
    batch, rows, d = x.shape
    f, mine = w_gate.shape[1], wq.shape[1]
    part, quarter = rows // 2, d // 4
    group, block = part // side, part // side // side
    low, dma = jnp.bfloat16, pltpu.SemaphoreType.DMA
    anywhere, vmem = pl.BlockSpec(memory_space=pl.ANY), pl.BlockSpec(memory_space=pltpu.VMEM)
    angle = np.arange(rows)[:, None] * float(THETA) ** (-np.arange(HEAD // 2) / (HEAD // 2))
    cos, sin = np.cos(angle).astype(np.float32), np.sin(angle).astype(np.float32)
    flops = 2 * batch * rows * d * (3 * f + 3 * mine)
    return pl.pallas_call(
        functools.partial(_layer, side),
        out_shape=jax.ShapeDtypeStruct(x.shape, low),
        in_specs=[anywhere, anywhere, vmem, anywhere, anywhere, anywhere, anywhere, vmem, vmem, anywhere, anywhere, anywhere],
        out_specs=anywhere,
        scratch_shapes=[
            pltpu.VMEM((2, rows, d), jnp.float32),
            pltpu.VMEM((2, rows, d), low),
            pltpu.VMEM((rows, d), low),
            pltpu.VMEM((2, rows, f), low),
            pltpu.VMEM((2, d, WIDE), low),
            pltpu.VMEM((2, f, WIDE), low),
            pltpu.VMEM((2, 2, 4, side - 1, group, quarter), low),
            pltpu.VMEM((2, 2, 4, side - 1, block, quarter), low),
            pltpu.VMEM((2, 4, group, quarter), low),
            pltpu.VMEM((2, 4, block, quarter), low),
            pltpu.VMEM((batch, 2, 4, block, quarter), low),
            *[dma(s) for _ in range(4) for s in ((2, 4, side - 1), (2, 2, 4, side - 1))],
            dma((2, 2)), dma((2,)), dma((batch, 2, 4)), dma((3,)), dma((2, 2, 3)), dma((2, 2, 3)), dma((2, 2, 2)), dma((2, 2, 2, 2)), dma((2,)), dma((2,)), dma,
        ],
        compiler_params=pltpu.CompilerParams(collective_id=0, has_side_effects=True, vmem_limit_bytes=LIMIT),
        cost_estimate=pl.CostEstimate(flops=flops, transcendentals=batch * rows * f, bytes_accessed=6 * batch * d * f),
    )(x, x.reshape(batch, rows // block, block, d), jnp.stack([gain_a, gain]), wq, wk, wv, wo.reshape(4, -1, d), jnp.asarray(np.concatenate([cos, cos], 1)), jnp.asarray(np.concatenate([-sin, sin], 1)),
      w_gate, w_up, w_down)


def _copied(source, target, hold, in_sem, out_sem):
    n, deep = source.shape[0], hold.shape[0]

    def into(t):
        return pltpu.make_async_copy(source.at[t], hold.at[t % deep], in_sem.at[t % deep])

    def out_of(t):
        return pltpu.make_async_copy(hold.at[t % deep], target.at[t], out_sem.at[t % deep])

    for t in range(deep // 2):
        into(t).start()
    for t in range(n):
        ahead = t + deep // 2
        if ahead < n:
            if ahead >= deep:
                out_of(ahead - deep).wait()
            into(ahead).start()
        into(t).wait()
        out_of(t).start()
    for t in range(max(n - deep, 0), n):
        out_of(t).wait()


def copied(y):
    batch, rows, d = y.shape
    pieces = y.reshape(batch * 4, rows // 4, d)
    deep = 12
    anywhere, dma = pl.BlockSpec(memory_space=pl.ANY), pltpu.SemaphoreType.DMA
    return pl.pallas_call(
        _copied,
        out_shape=jax.ShapeDtypeStruct(pieces.shape, y.dtype),
        in_specs=[anywhere],
        out_specs=anywhere,
        scratch_shapes=[pltpu.VMEM((deep, *pieces.shape[1:]), y.dtype), dma((deep,)), dma((deep,))],
        compiler_params=pltpu.CompilerParams(vmem_limit_bytes=LIMIT),
        cost_estimate=pl.CostEstimate(flops=0, transcendentals=0, bytes_accessed=4 * y.size),
    )(pieces).reshape(y.shape)


def solution(mesh):
    side = round(mesh.shape["tp"] ** 0.5)
    tokens, whole, columns, rows_of = P("dp", None, None), P(None), P(None, "tp"), P("tp", None)
    return jax.shard_map(
        lambda *arguments: copied(layer(side, *arguments)),
        mesh=mesh,
        in_specs=(tokens, whole, columns, columns, columns, rows_of, whole, columns, columns, rows_of),
        out_specs=tokens,
        check_vma=False,
    )
```
